32 devices in a mesh: lon: 4 (over y, x), lat: 8 (over z, core).
Axes of the slice: x: 2, y: 2, z: 4, core: 2. Of those that a mesh axis runs over, the one named last changes fastest.
Arguments:
- spectrum: float32 [32, 512, 648], P('lon', 'lat'), may hold values from 0.01 to 1
- sea_mask: int32 [32, 512], P('lon', 'lat'), may hold values from 0 to 1, as said below
- ice_flags: int32 [32, 512], P('lon', 'lat'), may hold values 0 or 1
- wind_forcing: float32 [32, 512], P('lon', 'lat'), may hold values from 0.1 to 1.5
- group_speed: float32 [18], replicated, may hold values from 0.3 to 1
- coupling: bfloat16 [648, 648], replicated, may hold values from -0.25 to 0.25
Outputs:
- field: float32 [32, 512, 648], P('lon', 'lat')
The draws below stay inside these ranges and needn't reach their ends.
Inputs may be any that keep to these rules, and one draw needn't show every extreme that they name: `sea_mask`: each device's block of 8 x 64 cells holds at most 384 sea cells and at least 128; in every draw some block holds exactly 384.
All inputs are finite; a program needn't handle non-finite values. No bound on the sum of `ice_flags` on one device may be relied on, other than what follows from the above.
Results may differ from the reference program's by a relative error of at most 0.00079.
Values sent between devices are 32-bit elements; how exact they have to be, the bound alone decides.
A program may use at most 64 MiB of HBM per device.

```python
import math
import jax
import jax.numpy as jnp

DIRS = 36
FREQS = 18
BINS = 648
CX = 8
CY = 64
SEA_DEV = 384
STEPS = 4
NX = 32
NY = 512


def draw_sea_mask(key, part):
    blocks_x = NX // CX
    blocks_y = NY // CY
    cells = CX * CY
    blocks = blocks_x * blocks_y
    key_count, key_pick, key_order = jax.random.split(jax.random.fold_in(key, 11), 3)
    counts = jax.random.randint(key_count, (blocks,), SEA_DEV // 3, SEA_DEV + 1)
    chosen = jax.random.randint(key_pick, (), 0, blocks)
    counts = counts.at[chosen].set(SEA_DEV)
    scores = jax.random.randint(key_order, (blocks, cells), 0, 2 ** 20) * cells + jnp.arange(cells, dtype=jnp.int32)[None, :]
    order = jnp.argsort(scores, axis=1, stable=True)
    ranks = jnp.argsort(order, axis=1, stable=True)
    flags = (ranks < counts[:, None]).astype(jnp.int32)
    flags = flags.reshape(blocks_x, blocks_y, CX, CY).transpose(0, 2, 1, 3)
    return flags.reshape(NX, NY)


def set_ends(array, key, low, largest):
    dims = array.shape
    index_at = [jax.random.randint(jax.random.fold_in(key, axis), (), 0, dims[axis]) for axis in range(len(dims))]
    array = array.at[tuple(index_at)].set(low)
    longest = dims.index(max(dims))
    index_at[longest] = (index_at[longest] + 1) % dims[longest]
    return array.at[tuple(index_at)].set(largest)


def levels(key, shape, cuts, least, largest):
    gain = 1.0
    for dim, parts in cuts:
        heights = jax.random.uniform(jax.random.fold_in(jax.random.fold_in(key, 6), dim), (parts,), jnp.float32, least / len(cuts), largest / len(cuts))
        gain = gain * jnp.repeat(jnp.exp(heights), shape[dim] // parts).reshape((-1,) + (1,) * (len(shape) - 1 - dim))
    return gain


def noise(stream_key, extent, scale, limit, kind=jnp.bfloat16):
    return jnp.clip(scale * jax.random.normal(stream_key, extent, jnp.float32), -limit, limit).astype(kind)


def setup_inputs(seed: int = 0) -> dict:
    arg_keys = jax.random.split(jax.random.key(seed), 7)
    spectrum = jnp.clip(jnp.exp(math.log(1.0) - 4.6051702 * jax.random.uniform(arg_keys[0], (NX, NY, BINS), jnp.float32) ** levels(arg_keys[0], (NX, NY, BINS), ((0, 4), (1, 8)), -0.2, 0.2)), 0.01, 1.0)
    sea_mask = draw_sea_mask(jax.random.fold_in(arg_keys[6], 71), 0)
    ice_flags = set_ends((jax.random.randint(arg_keys[2], (NX, NY), 0, 4) < 1).astype(jnp.int32), jax.random.fold_in(arg_keys[2], 1), 0, 1)
    wind_forcing = jnp.clip(jnp.exp(math.log(1.5) - 2.7080502 * jax.random.uniform(arg_keys[3], (NX, NY), jnp.float32) ** levels(arg_keys[3], (NX, NY), ((0, 4), (1, 8)), -0.2, 0.2)), 0.1, 1.5)
    group_speed = jnp.clip(jax.random.uniform(arg_keys[4], (FREQS,), jnp.float32, 0.3, 1.0), 0.3, 1.0)
    coupling = noise(arg_keys[5], (BINS, BINS), BINS ** -0.5, 0.25)
    return {"spectrum": spectrum, "sea_mask": sea_mask, "ice_flags": ice_flags, "wind_forcing": wind_forcing, "group_speed": group_speed, "coupling": coupling}


time_step = 0.2
dissipation = 0.5


def speed_tables(rows, total_rows, group_speed, dirs):
    theta = (jnp.arange(dirs).astype(jnp.float32) + 0.5) * (2.0 * math.pi / dirs)
    latitude = (-60.0 + 120.0 * (rows.astype(jnp.float32) + 0.5) / total_rows) * (math.pi / 180.0)
    scaled = jnp.outer(jnp.cos(theta), group_speed).reshape(-1)
    along_x = (0.225 * scaled)[None, :] / jnp.cos(latitude)[:, None]
    along_y = 0.45 * jnp.outer(jnp.sin(theta), group_speed).reshape(-1)
    return along_x, along_y


def upwind(field, west, east, south, north, along_x, along_y):
    speed_x = along_x[None]
    result = field - jnp.maximum(speed_x, 0.0) * (field - west) - jnp.minimum(speed_x, 0.0) * (east - field)
    return result - jnp.maximum(along_y, 0.0) * (field - south) - jnp.minimum(along_y, 0.0) * (north - field)


def sources(advected, wind_forcing, ice_flags, coupling):
    shape = advected.shape
    energy = jnp.mean(advected, axis=-1, keepdims=True)
    flat = advected.reshape(-1, shape[-1]).astype(jnp.bfloat16)
    transfer = jnp.dot(flat, coupling, preferred_element_type=jnp.float32).reshape(shape)
    forcing = (wind_forcing * (1.0 - ice_flags.astype(jnp.float32)))[..., None]
    return advected + time_step * (forcing * advected + transfer - dissipation * energy * advected)


def reference(spectrum, sea_mask, ice_flags, wind_forcing, group_speed, coupling):
    sea = sea_mask.astype(jnp.float32)[..., None]
    along_x, along_y = speed_tables(jnp.arange(NY), NY, group_speed, DIRS)
    field = spectrum * sea
    for step in range(STEPS):
        west = jnp.roll(field, 1, axis=0)
        east = jnp.roll(field, -1, axis=0)
        edge = jnp.zeros_like(field[:, :1])
        south = jnp.concatenate([edge, field[:, :-1]], axis=1)
        north = jnp.concatenate([field[:, 1:], edge], axis=1)
        advected = upwind(field, west, east, south, north, along_x, along_y)
        field = sources(advected, wind_forcing, ice_flags, coupling) * sea
    return field
```

```python
import functools
import math

import jax
import jax.numpy as jnp
from jax import lax
from jax.experimental import pallas as pl
from jax.experimental.pallas import tpu as pltpu
from jax.sharding import PartitionSpec as P

DIRS = 36
STEPS = 4
LANES = 128
PAD = 8
CHUNKS = 4
MESH = pl.DeviceIdType.MESH

time_step = 0.2
dissipation = 0.5


def kernel(
    freqs, speed_hbm, sea_hbm, ice_hbm, wind_hbm, spectrum_ref, coupling_ref, out_ref,
    speed_ref, sea_ref, ice_ref, wind_ref,
    field, staged, weights, east_weights, raw_weights, rounded, kept, keep_x, push_x, push_y, grow, scale,
    east_out, east_in, west_out, west_in, north_out, north_in, south_out, south_in,
    load_sem, small_sem, weight_sem, lon_send, lon_recv, lat_send, lat_recv,
):
    columns, rows, bins = staged.shape
    tiles = field.shape[2]
    piece = rows // CHUNKS
    side_rows = piece // 2
    middle = (CHUNKS - 1) * piece
    ends_chunk = CHUNKS - 1
    middle_at = columns * piece
    mean_of = 1.0 / bins
    quarter, half, late = DIRS // 4 * freqs, DIRS // 2 * freqs, DIRS * 3 // 4 * freqs
    cut_w, cut_y, cut_e = quarter - LANES, half - 2 * LANES, late - 3 * LANES
    late_w = LANES - cut_e
    inside = 64 - late_w - cut_w
    tail = bins - (tiles - 1) * LANES

    lon, lat = lax.axis_index("lon"), lax.axis_index("lat")
    lons, lats = lax.axis_size("lon"), lax.axis_size("lat")
    east, west = lax.rem(lon + 1, lons), lax.rem(lon + lons - 1, lons)
    has_south, has_north = lat > 0, lat < lats - 1
    odd = lax.rem(lon, 2) == 1

    def width(t):
        return LANES if t < tiles - 1 else tail

    last = columns - 1
    edges, inner = [0, last], list(range(1, last))
    loads = [
        pltpu.make_async_copy(spectrum_ref.at[c], staged.at[c], load_sem.at[c])
        for c in range(columns)
    ]
    weight_load = pltpu.make_async_copy(coupling_ref, raw_weights, weight_sem)
    small = [
        pltpu.make_async_copy(source, target, small_sem.at[n])
        for n, (source, target) in enumerate(
            ((sea_hbm, sea_ref), (speed_hbm, speed_ref), (ice_hbm, ice_ref), (wind_hbm, wind_ref))
        )
    ]
    for copy in small:
        copy.start()
    for c in edges:
        loads[c].start()

    barrier = pltpu.get_barrier_semaphore()
    pl.semaphore_signal(barrier, inc=1, device_id=(east, lat), device_id_type=MESH)
    pl.semaphore_signal(barrier, inc=1, device_id=(west, lat), device_id_type=MESH)

    @pl.when(has_south)
    def _():
        pl.semaphore_signal(barrier, inc=1, device_id=(lon, lat - 1), device_id_type=MESH)

    @pl.when(has_north)
    def _():
        pl.semaphore_signal(barrier, inc=1, device_id=(lon, lat + 1), device_id_type=MESH)

    small[0].wait()
    sea = sea_ref[...].astype(jnp.float32)
    sea_rows = jnp.transpose(sea)
    for c in range(columns):
        scale[c] = jnp.broadcast_to(sea_rows[:, c : c + 1], (rows, LANES))

    lane = lax.broadcasted_iota(jnp.int32, (8, LANES), 1)
    lane_piece = lax.broadcasted_iota(jnp.int32, (piece, LANES), 1)
    lane_eight = lax.broadcasted_iota(jnp.int32, (8, LANES), 1)
    row_eight = lax.broadcasted_iota(jnp.int32, (8, LANES), 0)
    own_low = lane_eight // 4 == row_eight + 1
    own_high = lane_eight // 4 == row_eight + 9
    low_half = lane_eight < LANES // 2

    def turn(value, by):
        return pltpu.roll(value, by % LANES, 1)

    def gather_rest(upper, lower, start):
        base = (4 - start) % LANES
        up = pltpu.roll(upper, base, 1, stride=4, stride_axis=0)
        down = pltpu.roll(lower, base + 32, 1, stride=4, stride_axis=0)
        spread = jnp.where(own_low, up, 0.0) + jnp.where(own_high, down, 0.0)
        return jnp.sum(spread, axis=0, keepdims=True)

    def spread_rest(line, start):
        line = jnp.broadcast_to(line, (8, LANES))
        halves = []
        for part in range(2):
            value = turn(line, start - 4 - 32 * part)
            for i in range(1, 8):
                value = jnp.where(row_eight == i, turn(line, start - 4 - 4 * i - 32 * part), value)
            halves.append(value)
        return halves

    def lon_copy(step, side, k):
        out_buf, in_buf, to = ((east_out, west_in, east), (west_out, east_in, west))[side]
        return pltpu.make_async_remote_copy(
            src_ref=out_buf.at[step, k],
            dst_ref=in_buf.at[step, k],
            send_sem=lon_send.at[step, side, k],
            recv_sem=lon_recv.at[step, side, k],
            device_id=(to, lat),
            device_id_type=MESH,
        )

    def lat_copy(step, side):
        out_buf, in_buf, to = ((north_out, south_in, lat + 1), (south_out, north_in, lat - 1))[side]
        return pltpu.make_async_remote_copy(
            src_ref=out_buf.at[step],
            dst_ref=in_buf.at[step],
            send_sem=lat_send.at[step, side],
            recv_sem=lat_recv.at[step, side],
            device_id=(lon, to),
            device_id_type=MESH,
        )

    MIDDLE = [(side_rows, middle)]
    ENDS = [(0, side_rows), (rows - side_rows, side_rows)]

    def spans_of(k):
        return ENDS if k == ends_chunk else [(side_rows + k * piece, piece)]

    def join(parts):
        return parts[0] if len(parts) == 1 else jnp.concatenate(parts, axis=0)

    def read(b, c, t, spans, shift=0):
        return join([field[b, c, t, PAD + at + shift : PAD + at + shift + n, :] for at, n in spans])

    def write(b, c, t, spans, value):
        done = 0
        for at, n in spans:
            field[b, c, t, PAD + at : PAD + at + n, :] = value[done : done + n]
            done += n

    def table(ref, i, spans):
        return join([ref[i, at : at + n, :] for at, n in spans])

    def rounded_at(c, k):
        return c * piece if k == ends_chunk else middle_at + c * middle + k * piece

    def mixed(lane_of, first, fifth, third):
        fifths = jnp.where(lane_of < cut_w + inside, turn(fifth, cut_w), turn(fifth, 64))
        return jnp.where(lane_of < cut_w, first, jnp.where(lane_of < cut_e, fifths, third))

    def pack_east(step, k, zero, four, rest):
        buffer = east_out.at[step, k]
        buffer[0:16, :] = zero
        buffer[16:32, :] = four
        low, high = rest[0:8], rest[8:16]
        buffer[32:40, :] = jnp.where(low_half, turn(low, late_w), turn(high, late_w + 64))
        buffer[40:41, :] = gather_rest(low, high, 64 + inside)

    def pack_west(step, k, one, two, three):
        buffer = west_out.at[step, k]
        buffer[0:16, :] = two
        buffer[16:32, :] = jnp.where(lane_piece < cut_e, three, one)
        low, high = one[0:8], one[8:16]
        buffer[32:40, :] = jnp.where(low_half, turn(low, -cut_w), turn(high, 64 - cut_w))
        buffer[40:41, :] = gather_rest(low, high, 64 + cut_w)

    def send_north(step):
        b = step % 2
        edge = slice(PAD + rows - 1, PAD + rows)
        for c in range(columns):
            for i in range(3):
                north_out[step, i, c : c + 1, :] = field[b, c, i, edge, :]

        @pl.when(has_north)
        def _():
            lat_copy(step, 0).start()

    def send_south(step):
        b = step % 2
        low = lane[0:1] < cut_y
        edge = slice(PAD, PAD + 1)
        for c in range(columns):
            south_out[step, 0, c : c + 1, :] = jnp.where(
                low, field[b, c, 5, edge, :], field[b, c, 2, edge, :]
            )
            for i in range(1, 3):
                south_out[step, i, c : c + 1, :] = field[b, c, i + 2, edge, :]

        @pl.when(has_south)
        def _():
            lat_copy(step, 1).start()

    def take_south(step):
        b = step % 2

        @pl.when(has_south)
        def _():
            lat_copy(step, 0).wait_recv()
            for c in range(columns):
                for i in range(3):
                    field[b, c, i, PAD - 1 : PAD, :] = south_in[step, i, c : c + 1, :]

    def take_north(step):
        b = step % 2
        edge = slice(PAD + rows, PAD + rows + 1)

        @pl.when(has_north)
        def _():
            lat_copy(step, 1).wait_recv()
            for c in range(columns):
                for i, t in ((0, 2), (1, 3), (2, 4), (0, 5)):
                    field[b, c, t, edge, :] = north_in[step, i, c : c + 1, :]

    def west_halo(step, k):
        buffer = west_in.at[step, k]
        main = buffer[32:40, :]
        rest = spread_rest(buffer[40:41, :], inside)
        shared = jnp.concatenate([turn(main, -late_w), turn(main, 64 - late_w)], axis=0)
        ends = [
            jnp.where(lane_eight < inside, turn(main, 64 * part + inside - 64), rest[part])
            for part in range(2)
        ]
        return {
            0: buffer[0:16, :],
            1: shared,
            3: shared,
            4: buffer[16:32, :],
            5: jnp.concatenate(ends, axis=0),
        }

    def east_halo(step, k):
        buffer = east_in.at[step, k]
        main, shared = buffer[32:40, :], buffer[16:32, :]
        rest = spread_rest(buffer[40:41, :], 64 + cut_w)
        moved = [
            jnp.where(lane_eight < 64 + cut_w, turn(main, cut_w - 64 * part), rest[part])
            for part in range(2)
        ]
        moved = jnp.concatenate(moved, axis=0)
        return {1: jnp.where(lane_piece < cut_e, moved, shared), 2: buffer[0:16, :], 3: shared}

    def advect(b, c, t, spans, from_west, from_east):
        lanes = lax.broadcasted_iota(jnp.int32, (sum(n for _, n in spans), LANES), 1)
        if t == 1:
            beside = jnp.where(lanes < cut_w, from_west(t), from_east(t))
        elif t == 2:
            beside = from_east(t)
        elif t == 3:
            beside = jnp.where(lanes < cut_e, from_east(t), from_west(t))
        else:
            beside = from_west(t)
        if t < 2:
            along = read(b, c, t, spans, -1)
        elif t == 2:
            along = jnp.where(lanes < cut_y, read(b, c, t, spans, -1), read(b, c, t, spans, 1))
        else:
            along = read(b, c, t, spans, 1)
        return (
            table(keep_x, t, spans) * read(b, c, t, spans)
            + table(push_x, t, spans) * beside
            + push_y[t, 0:1, :] * along
        )

    def advect_cell(step, c, spans, row, from_west, from_east):
        b = step % 2
        values, total = [], None
        n = sum(count for _, count in spans)
        for t in range(tiles):
            value = advect(b, c, t, spans, from_west, from_east)
            values.append(value)
            rounded[row : row + n, t * LANES : (t + 1) * LANES] = value.astype(jnp.bfloat16)
            total = value if total is None else total + value
        energy = jnp.sum(total, axis=1, keepdims=True) * mean_of
        growth = table(grow, c, spans) - (time_step * dissipation) * energy * table(scale, c, spans)
        return values, growth

    def advect_edge(step, side, k, row):
        b, spans = step % 2, spans_of(k)
        if side == 0:
            c, halo = 0, west_halo(step, k)
            return advect_cell(
                step, c, spans, row, lambda t: halo[t], lambda t: read(b, 1, t, spans)
            )
        c, halo = last, east_halo(step, k)
        return advect_cell(
            step, c, spans, row, lambda t: read(b, last - 1, t, spans), lambda t: halo[t]
        )

    def keep(c, spans, value):
        done = 0
        for at, n in spans:
            kept[c, at : at + n, :] = value[done : done + n]
            done += n

    def prepare(step, ends, group):
        b, spans = step % 2, ENDS if ends else MIDDLE
        deep = piece if ends else middle
        start = 0 if ends else middle_at
        for c in group:
            values, growth = advect_cell(
                step, c, spans, start + c * deep,
                lambda t, c=c: read(b, c - 1, t, spans), lambda t, c=c: read(b, c + 1, t, spans),
            )
            keep(c, spans, growth)
            for t in range(tiles):
                write(1 - b, c, t, spans, values[t])

    def edge(step, messages, filler=None):
        b = step % 2
        for side, k in messages:
            lon_copy(step, side, k).wait_recv()
        with jax.named_scope(f"edge#s={step}#k={messages[0][1]}#d={messages[0][0]}"):
            advected = []
            for side, k in messages:
                c, spans = 0 if side == 0 else last, spans_of(k)
                values, growth = advect_edge(step, side, k, rounded_at(c, k))
                keep(c, spans, growth)
                for t in range(tiles):
                    if t not in ((1, 2, 3), (0, 4))[side]:
                        write(1 - b, c, t, spans, values[t])
                if side == 1:
                    values[1] = mixed(lane_piece, values[1], values[5], values[3])
                advected.append((values, growth))
            products = []
            for side, k in messages:
                row = rounded_at(0 if side == 0 else last, k)
                part = weights[:, LANES : 4 * LANES] if side == 0 else east_weights[...]
                products.append(
                    jnp.dot(rounded[row : row + piece, :], part, preferred_element_type=jnp.float32)
                )
            if filler is not None:
                filler()
            for (side, k), (values, growth), transfer in zip(messages, advected, products):
                c, spans = 0 if side == 0 else last, spans_of(k)
                sea_here = time_step * table(scale, c, spans)
                sent = ((1, 2, 3), (0, 4, 1))[side]
                new = [
                    growth * values[t] + sea_here * transfer[:, i * LANES : (i + 1) * LANES]
                    for i, t in enumerate(sent)
                ]
                (pack_west, pack_east)[side](step + 1, k, *new)
                for t, value in list(zip(sent, new))[: 3 - side]:
                    write(1 - b, c, t, spans, value)
                lon_copy(step + 1, 1 - side, k).start()

    def block(step, ends):
        with jax.named_scope(f"block#s={step}#e={int(ends)}"):
            b, final = step % 2, step == STEPS - 1
            spans = ENDS if ends else MIDDLE
            deep = piece if ends else middle
            start = 0 if ends else middle_at
            first, count = (1, columns - 2) if final else (0, columns)
            transfer = jnp.dot(
                rounded[start + first * deep : start + (first + count) * deep, :], weights[...],
                preferred_element_type=jnp.float32,
            )
            for c in inner if final else range(columns):
                sea_here = time_step * table(scale, c, spans)
                growth = table(kept, c, spans)
                row = (c - first) * deep
                for t in (0, 4, 5) if c == 0 else (1, 2, 3, 5) if c == last else range(tiles):
                    moved = transfer[row : row + deep, t * LANES : (t + 1) * LANES]
                    value = growth * read(1 - b, c, t, spans) + sea_here * moved
                    if final:
                        emit(c, t, spans, value)
                    else:
                        write(1 - b, c, t, spans, value)

    def emit(c, t, spans, value):
        w, done = width(t), 0
        for at, n in spans:
            out_ref[c, at : at + n, t * LANES : t * LANES + w] = value[done : done + n, 0:w]
            done += n

    def finish(step, chunks):
        for side, k in chunks:
            lon_copy(step, side, k).wait_recv()
        with jax.named_scope(f"finish#n={len(chunks)}"):
            done = []
            for n, (side, k) in enumerate(chunks):
                done.append(advect_edge(step, side, k, n * piece))
            transfer = jnp.dot(
                rounded[0 : len(chunks) * piece, :], weights[...], preferred_element_type=jnp.float32
            )
            for n, (side, k) in enumerate(chunks):
                values, growth = done[n]
                c, spans = 0 if side == 0 else last, spans_of(k)
                sea_here = time_step * table(scale, c, spans)
                for t in range(tiles):
                    moved = transfer[n * piece : (n + 1) * piece, t * LANES : (t + 1) * LANES]
                    emit(c, t, spans, growth * values[t] + sea_here * moved)

    def by_side(step_of):
        @pl.when(odd)
        def _():
            step_of(1, 0)

        @pl.when(jnp.logical_not(odd))
        def _():
            step_of(0, 1)

    def take_column(c):
        for t in range(tiles):
            w = width(t)
            field[0, c, t, PAD : PAD + rows, 0:w] = (
                staged[c, :, t * LANES : t * LANES + w] * scale[c, :, 0:w]
            )

    for c in edges:
        field[0, c, tiles - 1, PAD : PAD + rows, :] = jnp.zeros((rows, LANES), jnp.float32)
    for c in edges:
        loads[c].wait()
    for c in inner:
        loads[c].start()
    weight_load.start()
    for c in edges:
        take_column(c)
    for k in range(CHUNKS):
        spans = spans_of(k)
        pack_west(0, k, *(read(0, 0, t, spans) for t in (1, 2, 3)))
        mine = [read(0, last, t, spans) for t in range(tiles)]
        pack_east(0, k, mine[0], mine[4], mixed(lane_piece, mine[1], mine[5], mine[3]))

    with jax.named_scope("barrier"):
        heard = 2 + has_south.astype(jnp.int32) + has_north.astype(jnp.int32)
        pl.semaphore_wait(barrier, heard)

    def send_first(first, second):
        for k in range(CHUNKS):
            lon_copy(0, 1 - first, k).start()
        for k in [ends_chunk] + list(range(CHUNKS - 1)):
            lon_copy(0, 1 - second, k).start()

    by_side(send_first)

    for copy in small[1:]:
        copy.wait()
    forcing = wind_ref[...] * (1.0 - ice_ref[...].astype(jnp.float32))
    growth = jnp.transpose(sea * (1.0 + time_step * forcing))
    for c in range(columns):
        grow[c] = jnp.broadcast_to(growth[:, c : c + 1], (rows, LANES))
    row = lax.broadcasted_iota(jnp.int32, (rows, LANES), 0) + lat * rows
    latitude = (-60.0 + 120.0 * (row.astype(jnp.float32) + 0.5) / (rows * lats)) * (math.pi / 180.0)
    inverse = 1.0 / jnp.cos(latitude)
    for t in range(tiles):
        number = (lane + t * LANES).astype(jnp.float32)
        direction = jnp.floor((number + 0.5) * (1.0 / freqs))
        freq = number - direction * freqs
        speed = jnp.zeros((8, LANES), jnp.float32)
        for f in range(freqs):
            speed = jnp.where(freq == f, speed_ref[f], speed)
        real = (lane + t * LANES) < bins
        theta = (direction + 0.5) * (2.0 * math.pi / DIRS)
        along_y = jnp.where(real, jnp.abs(0.45 * jnp.sin(theta) * speed), 0.0)
        along_x = jnp.where(real, jnp.abs(0.225 * jnp.cos(theta) * speed), 0.0)
        push_y[t] = along_y
        along_x = along_x[0:1] * inverse
        push_x[t] = along_x
        keep_x[t] = 1.0 - along_x - along_y[0:1]

    zero_row = jnp.zeros((1, LANES), jnp.float32)
    for c in range(columns):
        for t in range(tiles):
            for b in range(2):
                field[b, c, t, PAD - 1 : PAD, :] = zero_row
                field[b, c, t, PAD + rows : PAD + rows + 1, :] = zero_row
        if c in inner:
            field[0, c, tiles - 1, PAD : PAD + rows, :] = jnp.zeros((rows, LANES), jnp.float32)

    for c in inner:
        loads[c].wait()
        take_column(c)
    send_north(0)
    send_south(0)

    weight_load.wait()
    weights[...] = jnp.zeros_like(weights)
    weights[0:bins, 0:bins] = raw_weights[...]
    wide_lane = lax.broadcasted_iota(jnp.int32, (tiles * LANES, LANES), 1)
    east_weights[:, 0:LANES] = weights[:, 0:LANES]
    east_weights[:, LANES : 2 * LANES] = weights[:, 4 * LANES : 5 * LANES]
    first, third, fifth = (
        weights[:, t * LANES : (t + 1) * LANES].astype(jnp.float32) for t in (1, 3, 5)
    )
    east_weights[:, 2 * LANES : 3 * LANES] = mixed(wide_lane, first, fifth, third).astype(jnp.bfloat16)

    share = -(-len(inner) // (CHUNKS - 1))
    for step in range(STEPS):
        if step < STEPS - 1:

            def before(first, second):
                for k in range(CHUNKS - 1):
                    group = inner[k * share : (k + 1) * share]
                    edge(step, [(first, k)], lambda: prepare(step, False, group))
                take_south(step)
                take_north(step)
                edge(
                    step, [(first, ends_chunk), (second, ends_chunk)],
                    lambda: prepare(step, True, inner),
                )

            def after(first, second):
                for k in range(CHUNKS - 1):
                    edge(step, [(second, k)])

            by_side(before)
            block(step, True)
            send_south(step + 1)
            send_north(step + 1)
            by_side(after)
            block(step, False)
        else:
            prepare(step, False, inner)
            block(step, False)
            take_south(step)
            take_north(step)
            prepare(step, True, inner)
            block(step, True)

            def close(first, second):
                finish(step, [(first, k) for k in range(CHUNKS - 1)])
                finish(step, [(first, ends_chunk)] + [(second, k) for k in range(CHUNKS)])

            by_side(close)
    for step in range(STEPS):
        for k in range(CHUNKS):
            for side in range(2):
                lon_copy(step, side, k).wait_send()

        @pl.when(has_north)
        def _():
            lat_copy(step, 0).wait_send()

        @pl.when(has_south)
        def _():
            lat_copy(step, 1).wait_send()


def on_device(spectrum, sea_mask, ice_flags, wind_forcing, group_speed, coupling):
    columns, rows, bins = spectrum.shape
    tiles = -(-bins // LANES)
    wide = tiles * LANES
    piece = rows // CHUNKS
    hbm = pl.BlockSpec(memory_space=pltpu.HBM)
    operands = (group_speed, sea_mask, ice_flags, wind_forcing, spectrum, coupling)
    f32 = jnp.float32
    lon_buffer = pltpu.VMEM((STEPS, CHUNKS, 41, LANES), f32)
    lat_buffer = pltpu.VMEM((STEPS, 3, columns, LANES), f32)
    return pl.pallas_call(
        functools.partial(kernel, group_speed.shape[0]),
        out_shape=jax.ShapeDtypeStruct(spectrum.shape, spectrum.dtype),
        in_specs=[hbm] * 6,
        out_specs=pl.BlockSpec(memory_space=pltpu.VMEM),
        scratch_shapes=[
            pltpu.SMEM(group_speed.shape, f32),
            pltpu.VMEM((columns, rows), jnp.int32),
            pltpu.VMEM((columns, rows), jnp.int32),
            pltpu.VMEM((columns, rows), f32),
            pltpu.VMEM((2, columns, tiles, rows + 2 * PAD, LANES), f32),
            pltpu.VMEM((columns, rows, bins), f32),
            pltpu.VMEM((wide, wide), jnp.bfloat16),
            pltpu.VMEM((wide, 3 * LANES), jnp.bfloat16),
            pltpu.VMEM((bins, bins), jnp.bfloat16),
            pltpu.VMEM((columns * rows, wide), jnp.bfloat16),
            pltpu.VMEM((columns, rows, LANES), f32),
            pltpu.VMEM((tiles, rows, LANES), f32),
            pltpu.VMEM((tiles, rows, LANES), f32),
            pltpu.VMEM((tiles, 8, LANES), f32),
            pltpu.VMEM((columns, rows, LANES), f32),
            pltpu.VMEM((columns, rows, LANES), f32),
            lon_buffer, lon_buffer, lon_buffer, lon_buffer,
            lat_buffer, lat_buffer, lat_buffer, lat_buffer,
            pltpu.SemaphoreType.DMA((columns,)),
            pltpu.SemaphoreType.DMA((4,)),
            pltpu.SemaphoreType.DMA,
            pltpu.SemaphoreType.DMA((STEPS, 2, CHUNKS)),
            pltpu.SemaphoreType.DMA((STEPS, 2, CHUNKS)),
            pltpu.SemaphoreType.DMA((STEPS, 2)),
            pltpu.SemaphoreType.DMA((STEPS, 2)),
        ],
        compiler_params=pltpu.CompilerParams(
            collective_id=0, has_side_effects=True, vmem_limit_bytes=32 * 1024 * 1024
        ),
    )(*(pltpu.with_memory_space_constraint(x, pltpu.HBM) for x in operands))


def solution(mesh):
    placed = (P("lon", "lat", None), P("lon", "lat"), P("lon", "lat"), P("lon", "lat"), P(), P())
    return jax.shard_map(
        on_device, mesh=mesh, in_specs=placed, out_specs=P("lon", "lat", None), check_vma=False
    )
```

```python
import functools
import math

import jax
import jax.numpy as jnp
from jax import lax
from jax.experimental import pallas as pl
from jax.experimental.pallas import tpu as pltpu
from jax.sharding import PartitionSpec as P

DIRS = 36
STEPS = 4
LANES = 128
PAD = 8
CHUNKS = 4
MESH = pl.DeviceIdType.MESH

time_step = 0.2
dissipation = 0.5


def kernel(
    freqs, speed_hbm, sea_hbm, ice_hbm, wind_hbm, spectrum_ref, coupling_ref, out_ref,
    speed_ref, sea_ref, ice_ref, wind_ref,
    field, staged, weights, east_weights, raw_weights, rounded, kept, keep_x, push_x, push_y, grow, scale,
    east_out, east_in, west_out, west_in, north_out, north_in, south_out, south_in,
    load_sem, small_sem, weight_sem, lon_send, lon_recv, lat_send, lat_recv,
):
    columns, rows, bins = staged.shape
    tiles = field.shape[2]
    piece = rows // CHUNKS
    side_rows = piece // 2
    middle = (CHUNKS - 1) * piece
    ends_chunk = CHUNKS - 1
    middle_at = columns * piece
    mean_of = 1.0 / bins
    quarter, half, late = DIRS // 4 * freqs, DIRS // 2 * freqs, DIRS * 3 // 4 * freqs
    cut_w, cut_y, cut_e = quarter - LANES, half - 2 * LANES, late - 3 * LANES
    late_w = LANES - cut_e
    inside = 64 - late_w - cut_w
    tail = bins - (tiles - 1) * LANES

    lon, lat = lax.axis_index("lon"), lax.axis_index("lat")
    lons, lats = lax.axis_size("lon"), lax.axis_size("lat")
    east, west = lax.rem(lon + 1, lons), lax.rem(lon + lons - 1, lons)
    has_south, has_north = lat > 0, lat < lats - 1
    odd = lax.rem(lon, 2) == 1

    def width(t):
        return LANES if t < tiles - 1 else tail

    last = columns - 1
    edges, inner = [0, last], list(range(1, last))
    loads = [
        pltpu.make_async_copy(
            spectrum_ref.at[c], staged.at[c], load_sem.at[0 if c in edges else 1]
        )
        for c in range(columns)
    ]
    edge_loads, inner_loads = (
        pltpu.make_async_copy(
            spectrum_ref.at[0:count], staged.at[0:count], load_sem.at[n]
        )
        for n, count in enumerate((2, columns - 2))
    )
    weight_load = pltpu.make_async_copy(coupling_ref, raw_weights, weight_sem)
    small = [
        pltpu.make_async_copy(source, target, small_sem.at[n])
        for n, (source, target) in enumerate(
            ((sea_hbm, sea_ref), (speed_hbm, speed_ref), (ice_hbm, ice_ref), (wind_hbm, wind_ref))
        )
    ]
    barrier = pltpu.get_barrier_semaphore()
    pl.semaphore_signal(barrier, inc=1, device_id=(east, lat), device_id_type=MESH)
    pl.semaphore_signal(barrier, inc=1, device_id=(west, lat), device_id_type=MESH)

    @pl.when(has_south)
    def _():
        pl.semaphore_signal(barrier, inc=1, device_id=(lon, lat - 1), device_id_type=MESH)

    @pl.when(has_north)
    def _():
        pl.semaphore_signal(barrier, inc=1, device_id=(lon, lat + 1), device_id_type=MESH)

    for copy in small:
        copy.start()
    for c in edges:
        loads[c].start()

    small[0].wait()
    sea = sea_ref[...].astype(jnp.float32)
    sea_rows = jnp.transpose(sea)
    for c in range(columns):
        scale[c] = jnp.broadcast_to(sea_rows[:, c : c + 1], (rows, LANES))

    lane = lax.broadcasted_iota(jnp.int32, (8, LANES), 1)
    lane_piece = lax.broadcasted_iota(jnp.int32, (piece, LANES), 1)
    lane_eight = lax.broadcasted_iota(jnp.int32, (8, LANES), 1)
    row_eight = lax.broadcasted_iota(jnp.int32, (8, LANES), 0)
    own_low = lane_eight // 4 == row_eight + 1
    own_high = lane_eight // 4 == row_eight + 9
    low_half = lane_eight < LANES // 2

    def turn(value, by):
        return pltpu.roll(value, by % LANES, 1)

    def gather_rest(upper, lower, start):
        base = (4 - start) % LANES
        up = pltpu.roll(upper, base, 1, stride=4, stride_axis=0)
        down = pltpu.roll(lower, base + 32, 1, stride=4, stride_axis=0)
        spread = jnp.where(own_low, up, 0.0) + jnp.where(own_high, down, 0.0)
        return jnp.sum(spread, axis=0, keepdims=True)

    def spread_rest(line, start):
        line = jnp.broadcast_to(line, (8, LANES))
        halves = []
        for part in range(2):
            value = turn(line, start - 4 - 32 * part)
            for i in range(1, 8):
                value = jnp.where(row_eight == i, turn(line, start - 4 - 4 * i - 32 * part), value)
            halves.append(value)
        return halves

    def lon_copy(step, side, k):
        out_buf, in_buf, to = ((east_out, west_in, east), (west_out, east_in, west))[side]
        return pltpu.make_async_remote_copy(
            src_ref=out_buf.at[step, k],
            dst_ref=in_buf.at[step, k],
            send_sem=lon_send.at[side],
            recv_sem=lon_recv.at[step % 2, side, k],
            device_id=(to, lat),
            device_id_type=MESH,
        )

    def lat_copy(step, side):
        out_buf, in_buf, to = ((north_out, south_in, lat + 1), (south_out, north_in, lat - 1))[side]
        return pltpu.make_async_remote_copy(
            src_ref=out_buf.at[step],
            dst_ref=in_buf.at[step],
            send_sem=lat_send.at[side],
            recv_sem=lat_recv.at[step % 2, side],
            device_id=(lon, to),
            device_id_type=MESH,
        )

    MIDDLE = [(side_rows, middle)]
    ENDS = [(0, side_rows), (rows - side_rows, side_rows)]

    def spans_of(k):
        return ENDS if k == ends_chunk else [(side_rows + k * piece, piece)]

    def join(parts):
        return parts[0] if len(parts) == 1 else jnp.concatenate(parts, axis=0)

    def read(b, c, t, spans, shift=0):
        return join([field[b, c, t, PAD + at + shift : PAD + at + shift + n, :] for at, n in spans])

    def write(b, c, t, spans, value):
        done = 0
        for at, n in spans:
            field[b, c, t, PAD + at : PAD + at + n, :] = value[done : done + n]
            done += n

    def table(ref, i, spans):
        return join([ref[i, at : at + n, :] for at, n in spans])

    def rounded_at(c, k):
        return c * piece if k == ends_chunk else middle_at + c * middle + k * piece

    def mixed(lane_of, first, fifth, third):
        fifths = jnp.where(lane_of < cut_w + inside, turn(fifth, cut_w), turn(fifth, 64))
        return jnp.where(lane_of < cut_w, first, jnp.where(lane_of < cut_e, fifths, third))

    def pack_east(step, k, rest, zero, four):
        buffer = east_out.at[step, k]
        buffer[0:16, :] = zero
        buffer[16:32, :] = four
        low, high = rest[0:8], rest[8:16]
        buffer[32:40, :] = jnp.where(low_half, turn(low, late_w), turn(high, late_w + 64))
        buffer[40:41, :] = gather_rest(low, high, 64 + inside)

    def pack_west(step, k, one, two, three):
        buffer = west_out.at[step, k]
        buffer[0:16, :] = two
        buffer[16:32, :] = jnp.where(lane_piece < cut_e, three, one)
        low, high = one[0:8], one[8:16]
        buffer[32:40, :] = jnp.where(low_half, turn(low, -cut_w), turn(high, 64 - cut_w))
        buffer[40:41, :] = gather_rest(low, high, 64 + cut_w)

    def send_north(step):
        b = step % 2
        edge = slice(PAD + rows - 1, PAD + rows)
        for c in range(columns):
            for i in range(3):
                north_out[step, i, c : c + 1, :] = field[b, c, i, edge, :]

        @pl.when(has_north)
        def _():
            lat_copy(step, 0).start()

    def send_south(step):
        b = step % 2
        low = lane[0:1] < cut_y
        edge = slice(PAD, PAD + 1)
        for c in range(columns):
            south_out[step, 0, c : c + 1, :] = jnp.where(
                low, field[b, c, 5, edge, :], field[b, c, 2, edge, :]
            )
            for i in range(1, 3):
                south_out[step, i, c : c + 1, :] = field[b, c, i + 2, edge, :]

        @pl.when(has_south)
        def _():
            lat_copy(step, 1).start()

    def take_south(step):
        b = step % 2

        @pl.when(has_south)
        def _():
            lat_copy(step, 0).wait_recv()
            for c in range(columns):
                for i in range(3):
                    field[b, c, i, PAD - 1 : PAD, :] = south_in[step, i, c : c + 1, :]

    def take_north(step):
        b = step % 2
        edge = slice(PAD + rows, PAD + rows + 1)

        @pl.when(has_north)
        def _():
            lat_copy(step, 1).wait_recv()
            for c in range(columns):
                for i, t in ((0, 2), (1, 3), (2, 4), (0, 5)):
                    field[b, c, t, edge, :] = north_in[step, i, c : c + 1, :]

    def west_halo(step, k):
        buffer = west_in.at[step, k]
        main = buffer[32:40, :]
        rest = spread_rest(buffer[40:41, :], inside)
        shared = jnp.concatenate([turn(main, -late_w), turn(main, 64 - late_w)], axis=0)
        ends = [
            jnp.where(lane_eight < inside, turn(main, 64 * part + inside - 64), rest[part])
            for part in range(2)
        ]
        return {
            0: buffer[0:16, :],
            1: shared,
            3: shared,
            4: buffer[16:32, :],
            5: jnp.concatenate(ends, axis=0),
        }

    def east_halo(step, k):
        buffer = east_in.at[step, k]
        main, shared = buffer[32:40, :], buffer[16:32, :]
        rest = spread_rest(buffer[40:41, :], 64 + cut_w)
        moved = [
            jnp.where(lane_eight < 64 + cut_w, turn(main, cut_w - 64 * part), rest[part])
            for part in range(2)
        ]
        moved = jnp.concatenate(moved, axis=0)
        return {1: jnp.where(lane_piece < cut_e, moved, shared), 2: buffer[0:16, :], 3: shared}

    def advect(b, c, t, spans, from_west, from_east):
        lanes = lax.broadcasted_iota(jnp.int32, (sum(n for _, n in spans), LANES), 1)
        if t == 1:
            beside = jnp.where(lanes < cut_w, from_west(t), from_east(t))
        elif t == 2:
            beside = from_east(t)
        elif t == 3:
            beside = jnp.where(lanes < cut_e, from_east(t), from_west(t))
        else:
            beside = from_west(t)
        if t < 2:
            along = read(b, c, t, spans, -1)
        elif t == 2:
            along = jnp.where(lanes < cut_y, read(b, c, t, spans, -1), read(b, c, t, spans, 1))
        else:
            along = read(b, c, t, spans, 1)
        return (
            table(keep_x, t, spans) * read(b, c, t, spans)
            + table(push_x, t, spans) * beside
            + push_y[t, 0:1, :] * along
        )

    def advect_cell(step, c, spans, row, from_west, from_east):
        b = step % 2
        values, total = [], None
        n = sum(count for _, count in spans)
        for t in range(tiles):
            value = advect(b, c, t, spans, from_west, from_east)
            values.append(value)
            rounded[row : row + n, t * LANES : (t + 1) * LANES] = value.astype(jnp.bfloat16)
            total = value if total is None else total + value
        energy = jnp.sum(total, axis=1, keepdims=True) * mean_of
        growth = table(grow, c, spans) - (time_step * dissipation) * energy * table(scale, c, spans)
        return values, growth

    def advect_edge(step, side, k, row):
        b, spans = step % 2, spans_of(k)
        if side == 0:
            c, halo = 0, west_halo(step, k)
            return advect_cell(
                step, c, spans, row, lambda t: halo[t], lambda t: read(b, 1, t, spans)
            )
        c, halo = last, east_halo(step, k)
        return advect_cell(
            step, c, spans, row, lambda t: read(b, last - 1, t, spans), lambda t: halo[t]
        )

    def keep(c, spans, value):
        done = 0
        for at, n in spans:
            kept[c, at : at + n, :] = value[done : done + n]
            done += n

    def prepare(step, ends, group):
        b, spans = step % 2, ENDS if ends else MIDDLE
        deep = piece if ends else middle
        start = 0 if ends else middle_at
        for c in group:
            values, growth = advect_cell(
                step, c, spans, start + c * deep,
                lambda t, c=c: read(b, c - 1, t, spans), lambda t, c=c: read(b, c + 1, t, spans),
            )
            keep(c, spans, growth)
            for t in range(tiles):
                write(1 - b, c, t, spans, values[t])

    def edge(step, messages, filler=None):
        b = step % 2
        for side, k in messages:
            lon_copy(step, side, k).wait_recv()
        with jax.named_scope(f"edge#s={step}#k={messages[0][1]}#d={messages[0][0]}"):
            advected = []
            for side, k in messages:
                c, spans = 0 if side == 0 else last, spans_of(k)
                values, growth = advect_edge(step, side, k, rounded_at(c, k))
                keep(c, spans, growth)
                for t in range(tiles):
                    if t not in ((1, 2, 3), (0, 4))[side]:
                        write(1 - b, c, t, spans, values[t])
                if side == 1:
                    values[1] = mixed(lane_piece, values[1], values[5], values[3])
                advected.append((values, growth))
            products = []
            for side, k in messages:
                row = rounded_at(0 if side == 0 else last, k)
                part, at = (weights, LANES) if side == 0 else (east_weights, 0)
                products.append([
                    jnp.dot(
                        rounded[row : row + piece, :], part[:, at + i * LANES : at + (i + 1) * LANES],
                        preferred_element_type=jnp.float32,
                    )
                    for i in range(3)
                ])
            if filler is not None:
                filler()
            for (side, k), (values, growth), transfer in zip(messages, advected, products):
                c, spans = 0 if side == 0 else last, spans_of(k)
                sea_here = time_step * table(scale, c, spans)
                sent = ((1, 2, 3), (1, 0, 4))[side]
                new = [
                    growth * values[t] + sea_here * transfer[i]
                    for i, t in enumerate(sent)
                ]
                (pack_west, pack_east)[side](step + 1, k, *new)
                for t, value in list(zip(sent, new))[side:]:
                    write(1 - b, c, t, spans, value)
                lon_copy(step + 1, 1 - side, k).start()

    def block(step, ends):
        with jax.named_scope(f"block#s={step}#e={int(ends)}"):
            b, final = step % 2, step == STEPS - 1
            spans = ENDS if ends else MIDDLE
            deep = piece if ends else middle
            start = 0 if ends else middle_at
            first, count = (1, columns - 2) if final else (0, columns)
            transfer = jnp.dot(
                rounded[start + first * deep : start + (first + count) * deep, :], weights[...],
                preferred_element_type=jnp.float32,
            )
            for c in inner if final else range(columns):
                sea_here = time_step * table(scale, c, spans)
                growth = table(kept, c, spans)
                row = (c - first) * deep
                for t in (0, 4, 5) if c == 0 else (1, 2, 3, 5) if c == last else range(tiles):
                    moved = transfer[row : row + deep, t * LANES : (t + 1) * LANES]
                    value = growth * read(1 - b, c, t, spans) + sea_here * moved
                    if final:
                        emit(c, t, spans, value)
                    else:
                        write(1 - b, c, t, spans, value)

    def emit(c, t, spans, value):
        w, done = width(t), 0
        for at, n in spans:
            out_ref[c, at : at + n, t * LANES : t * LANES + w] = value[done : done + n, 0:w]
            done += n

    def finish(step, chunks):
        for side, k in chunks:
            lon_copy(step, side, k).wait_recv()
        with jax.named_scope(f"finish#n={len(chunks)}"):
            done = []
            for n, (side, k) in enumerate(chunks):
                done.append(advect_edge(step, side, k, n * piece))
            transfer = jnp.dot(
                rounded[0 : len(chunks) * piece, :], weights[...], preferred_element_type=jnp.float32
            )
            for n, (side, k) in enumerate(chunks):
                values, growth = done[n]
                c, spans = 0 if side == 0 else last, spans_of(k)
                sea_here = time_step * table(scale, c, spans)
                for t in range(tiles):
                    moved = transfer[n * piece : (n + 1) * piece, t * LANES : (t + 1) * LANES]
                    emit(c, t, spans, growth * values[t] + sea_here * moved)

    def by_side(step_of):
        @pl.when(odd)
        def _():
            step_of(1, 0)

        @pl.when(jnp.logical_not(odd))
        def _():
            step_of(0, 1)

    def take_column(c):
        for t in range(tiles):
            w = width(t)
            field[0, c, t, PAD : PAD + rows, 0:w] = (
                staged[c, :, t * LANES : t * LANES + w] * scale[c, :, 0:w]
            )

    for c in edges:
        field[0, c, tiles - 1, PAD : PAD + rows, :] = jnp.zeros((rows, LANES), jnp.float32)
    edge_loads.wait()
    for c in inner:
        loads[c].start()
    weight_load.start()
    for c in edges:
        take_column(c)
    for k in range(CHUNKS):
        spans = spans_of(k)
        pack_west(0, k, *(read(0, 0, t, spans) for t in (1, 2, 3)))
        mine = [read(0, last, t, spans) for t in range(tiles)]
        pack_east(0, k, mixed(lane_piece, mine[1], mine[5], mine[3]), mine[0], mine[4])

    with jax.named_scope("barrier"):
        heard = 2 + has_south.astype(jnp.int32) + has_north.astype(jnp.int32)
        pl.semaphore_wait(barrier, heard)

    def send_first(first, second):
        for k in range(CHUNKS):
            lon_copy(0, 1 - first, k).start()
        for k in [ends_chunk] + list(range(CHUNKS - 1)):
            lon_copy(0, 1 - second, k).start()

    by_side(send_first)

    for copy in small[1:]:
        copy.wait()
    forcing = wind_ref[...] * (1.0 - ice_ref[...].astype(jnp.float32))
    growth = jnp.transpose(sea * (1.0 + time_step * forcing))
    for c in range(columns):
        grow[c] = jnp.broadcast_to(growth[:, c : c + 1], (rows, LANES))
    row = lax.broadcasted_iota(jnp.int32, (rows, LANES), 0) + lat * rows
    latitude = (-60.0 + 120.0 * (row.astype(jnp.float32) + 0.5) / (rows * lats)) * (math.pi / 180.0)
    inverse = 1.0 / jnp.cos(latitude)
    for t in range(tiles):
        number = (lane + t * LANES).astype(jnp.float32)
        direction = jnp.floor((number + 0.5) * (1.0 / freqs))
        freq = number - direction * freqs
        speed = jnp.zeros((8, LANES), jnp.float32)
        for f in range(freqs):
            speed = jnp.where(freq == f, speed_ref[f], speed)
        real = (lane + t * LANES) < bins
        theta = (direction + 0.5) * (2.0 * math.pi / DIRS)
        along_y = jnp.where(real, jnp.abs(0.45 * jnp.sin(theta) * speed), 0.0)
        along_x = jnp.where(real, jnp.abs(0.225 * jnp.cos(theta) * speed), 0.0)
        push_y[t] = along_y
        along_x = along_x[0:1] * inverse
        push_x[t] = along_x
        keep_x[t] = 1.0 - along_x - along_y[0:1]

    zero_row = jnp.zeros((1, LANES), jnp.float32)
    for c in range(columns):
        for t in range(tiles):
            for b in range(2):
                field[b, c, t, PAD - 1 : PAD, :] = zero_row
                field[b, c, t, PAD + rows : PAD + rows + 1, :] = zero_row
        if c in inner:
            field[0, c, tiles - 1, PAD : PAD + rows, :] = jnp.zeros((rows, LANES), jnp.float32)

    inner_loads.wait()
    for c in inner:
        take_column(c)
    send_north(0)
    send_south(0)

    weight_load.wait()
    weights[...] = jnp.zeros_like(weights)
    weights[0:bins, 0:bins] = raw_weights[...]
    wide_lane = lax.broadcasted_iota(jnp.int32, (tiles * LANES, LANES), 1)
    east_weights[:, LANES : 2 * LANES] = weights[:, 0:LANES]
    east_weights[:, 2 * LANES : 3 * LANES] = weights[:, 4 * LANES : 5 * LANES]
    first, third, fifth = (
        weights[:, t * LANES : (t + 1) * LANES].astype(jnp.float32) for t in (1, 3, 5)
    )
    east_weights[:, 0:LANES] = mixed(wide_lane, first, fifth, third).astype(jnp.bfloat16)

    share = -(-len(inner) // (CHUNKS - 1))
    for step in range(STEPS):
        if step < STEPS - 1:

            def before(first, second):
                for k in range(CHUNKS - 1):
                    group = inner[k * share : (k + 1) * share]
                    edge(step, [(first, k)], lambda: prepare(step, False, group))
                take_south(step)
                take_north(step)
                edge(
                    step, [(first, ends_chunk), (second, ends_chunk)],
                    lambda: prepare(step, True, inner),
                )

            def after(first, second):
                for k in range(CHUNKS - 1):
                    edge(step, [(second, k)])

            by_side(before)
            block(step, True)
            send_south(step + 1)
            send_north(step + 1)
            by_side(after)
            block(step, False)
        else:
            prepare(step, False, inner)
            block(step, False)
            take_south(step)
            take_north(step)
            prepare(step, True, inner)
            block(step, True)

            def close(first, second):
                finish(step, [(first, k) for k in range(CHUNKS - 1)])
                finish(step, [(first, ends_chunk)] + [(second, k) for k in range(CHUNKS)])

            by_side(close)
    for side, (out_buf, in_buf) in enumerate(((east_out, west_in), (west_out, east_in))):
        pltpu.make_async_remote_copy(
            src_ref=out_buf, dst_ref=in_buf, send_sem=lon_send.at[side],
            recv_sem=lon_recv.at[0, side, 0], device_id=(east, lat), device_id_type=MESH,
        ).wait_send()
    for side, (out_buf, in_buf, there) in enumerate(
        ((north_out, south_in, has_north), (south_out, north_in, has_south))
    ):

        @pl.when(there)
        def _():
            pltpu.make_async_remote_copy(
                src_ref=out_buf, dst_ref=in_buf, send_sem=lat_send.at[side],
                recv_sem=lat_recv.at[0, side], device_id=(east, lat), device_id_type=MESH,
            ).wait_send()


def on_device(spectrum, sea_mask, ice_flags, wind_forcing, group_speed, coupling):
    columns, rows, bins = spectrum.shape
    tiles = -(-bins // LANES)
    wide = tiles * LANES
    piece = rows // CHUNKS
    hbm = pl.BlockSpec(memory_space=pltpu.HBM)
    operands = (group_speed, sea_mask, ice_flags, wind_forcing, spectrum, coupling)
    f32 = jnp.float32
    lon_buffer = pltpu.VMEM((STEPS, CHUNKS, 41, LANES), f32)
    lat_buffer = pltpu.VMEM((STEPS, 3, columns, LANES), f32)
    return pl.pallas_call(
        functools.partial(kernel, group_speed.shape[0]),
        out_shape=jax.ShapeDtypeStruct(spectrum.shape, spectrum.dtype),
        in_specs=[hbm] * 6,
        out_specs=pl.BlockSpec(memory_space=pltpu.VMEM),
        scratch_shapes=[
            pltpu.SMEM(group_speed.shape, f32),
            pltpu.VMEM((columns, rows), jnp.int32),
            pltpu.VMEM((columns, rows), jnp.int32),
            pltpu.VMEM((columns, rows), f32),
            pltpu.VMEM((2, columns, tiles, rows + 2 * PAD, LANES), f32),
            pltpu.VMEM((columns, rows, bins), f32),
            pltpu.VMEM((wide, wide), jnp.bfloat16),
            pltpu.VMEM((wide, 3 * LANES), jnp.bfloat16),
            pltpu.VMEM((bins, bins), jnp.bfloat16),
            pltpu.VMEM((columns * rows, wide), jnp.bfloat16),
            pltpu.VMEM((columns, rows, LANES), f32),
            pltpu.VMEM((tiles, rows, LANES), f32),
            pltpu.VMEM((tiles, rows, LANES), f32),
            pltpu.VMEM((tiles, 8, LANES), f32),
            pltpu.VMEM((columns, rows, LANES), f32),
            pltpu.VMEM((columns, rows, LANES), f32),
            lon_buffer, lon_buffer, lon_buffer, lon_buffer,
            lat_buffer, lat_buffer, lat_buffer, lat_buffer,
            pltpu.SemaphoreType.DMA((2,)),
            pltpu.SemaphoreType.DMA((4,)),
            pltpu.SemaphoreType.DMA,
            pltpu.SemaphoreType.DMA((2,)),
            pltpu.SemaphoreType.DMA((2, 2, CHUNKS)),
            pltpu.SemaphoreType.DMA((2,)),
            pltpu.SemaphoreType.DMA((2, 2)),
        ],
        compiler_params=pltpu.CompilerParams(
            collective_id=0, has_side_effects=True, vmem_limit_bytes=32 * 1024 * 1024
        ),
    )(*(pltpu.with_memory_space_constraint(x, pltpu.HBM) for x in operands))


def solution(mesh):
    placed = (P("lon", "lat", None), P("lon", "lat"), P("lon", "lat"), P("lon", "lat"), P(), P())
    return jax.shard_map(
        on_device, mesh=mesh, in_specs=placed, out_specs=P("lon", "lat", None), check_vma=False
    )
```

```python
import functools
import math

import jax
import jax.numpy as jnp
from jax import lax
from jax.experimental import pallas as pl
from jax.experimental.pallas import tpu as pltpu
from jax.sharding import PartitionSpec as P

DIRS = 36
STEPS = 4
LANES = 128
PAD = 8
CHUNKS = 4
MESH = pl.DeviceIdType.MESH

time_step = 0.2
dissipation = 0.5


def kernel(
    freqs, speed_hbm, sea_hbm, ice_hbm, wind_hbm, spectrum_ref, coupling_ref, out_ref,
    speed_ref, sea_ref, ice_ref, wind_ref,
    field, staged, weights, east_weights, raw_weights, rounded, kept, keep_x, push_x, push_y, grow, scale,
    east_out, east_in, west_out, west_in, north_out, north_in, south_out, south_in,
    load_sem, small_sem, weight_sem, lon_send, lon_recv, lat_send, lat_recv,
):
    columns, rows, bins = staged.shape
    tiles = field.shape[2]
    piece = rows // CHUNKS
    side_rows = piece // 2
    middle = (CHUNKS - 1) * piece
    ends_chunk = CHUNKS - 1
    middle_at = columns * piece
    mean_of = 1.0 / bins
    quarter, half, late = DIRS // 4 * freqs, DIRS // 2 * freqs, DIRS * 3 // 4 * freqs
    cut_w, cut_y, cut_e = quarter - LANES, half - 2 * LANES, late - 3 * LANES
    late_w = LANES - cut_e
    inside = 64 - late_w - cut_w
    tail = bins - (tiles - 1) * LANES

    lon, lat = lax.axis_index("lon"), lax.axis_index("lat")
    lons, lats = lax.axis_size("lon"), lax.axis_size("lat")
    east, west = lax.rem(lon + 1, lons), lax.rem(lon + lons - 1, lons)
    has_south, has_north = lat > 0, lat < lats - 1
    odd = lax.rem(lon, 2) == 1

    def width(t):
        return LANES if t < tiles - 1 else tail

    last = columns - 1
    edges, inner = [0, last], list(range(1, last))
    loads = [
        pltpu.make_async_copy(
            spectrum_ref.at[c], staged.at[c], load_sem.at[0 if c in edges else 1]
        )
        for c in range(columns)
    ]
    edge_loads, inner_loads = (
        pltpu.make_async_copy(
            spectrum_ref.at[0:count], staged.at[0:count], load_sem.at[n]
        )
        for n, count in enumerate((2, columns - 2))
    )
    weight_load = pltpu.make_async_copy(coupling_ref, raw_weights, weight_sem)
    small = [
        pltpu.make_async_copy(source, target, small_sem.at[n])
        for n, (source, target) in enumerate(
            ((sea_hbm, sea_ref), (speed_hbm, speed_ref), (ice_hbm, ice_ref), (wind_hbm, wind_ref))
        )
    ]
    barrier = pltpu.get_barrier_semaphore()
    pl.semaphore_signal(barrier, inc=1, device_id=(east, lat), device_id_type=MESH)
    pl.semaphore_signal(barrier, inc=1, device_id=(west, lat), device_id_type=MESH)

    @pl.when(has_south)
    def _():
        pl.semaphore_signal(barrier, inc=1, device_id=(lon, lat - 1), device_id_type=MESH)

    @pl.when(has_north)
    def _():
        pl.semaphore_signal(barrier, inc=1, device_id=(lon, lat + 1), device_id_type=MESH)

    for copy in small:
        copy.start()
    for c in edges:
        loads[c].start()

    small[0].wait()
    sea = sea_ref[...].astype(jnp.float32)
    sea_rows = jnp.transpose(sea)
    for c in range(columns):
        scale[c] = jnp.broadcast_to(sea_rows[:, c : c + 1], (rows, LANES))

    lane = lax.broadcasted_iota(jnp.int32, (8, LANES), 1)
    lane_piece = lax.broadcasted_iota(jnp.int32, (piece, LANES), 1)
    lane_eight = lax.broadcasted_iota(jnp.int32, (8, LANES), 1)
    row_eight = lax.broadcasted_iota(jnp.int32, (8, LANES), 0)
    own_low = lane_eight // 4 == row_eight + 1
    own_high = lane_eight // 4 == row_eight + 9
    low_half = lane_eight < LANES // 2

    def turn(value, by):
        return pltpu.roll(value, by % LANES, 1)

    def gather_rest(upper, lower, start):
        base = (4 - start) % LANES
        up = pltpu.roll(upper, base, 1, stride=4, stride_axis=0)
        down = pltpu.roll(lower, base + 32, 1, stride=4, stride_axis=0)
        spread = jnp.where(own_low, up, 0.0) + jnp.where(own_high, down, 0.0)
        return jnp.sum(spread, axis=0, keepdims=True)

    def spread_rest(line, start):
        line = jnp.broadcast_to(line, (8, LANES))
        halves = []
        for part in range(2):
            value = turn(line, start - 4 - 32 * part)
            for i in range(1, 8):
                value = jnp.where(row_eight == i, turn(line, start - 4 - 4 * i - 32 * part), value)
            halves.append(value)
        return halves

    def lon_copy(step, side, k):
        out_buf, in_buf, to = ((east_out, west_in, east), (west_out, east_in, west))[side]
        return pltpu.make_async_remote_copy(
            src_ref=out_buf.at[step, k],
            dst_ref=in_buf.at[step, k],
            send_sem=lon_send.at[side],
            recv_sem=lon_recv.at[step % 2, side, k],
            device_id=(to, lat),
            device_id_type=MESH,
        )

    def lat_copy(step, side):
        out_buf, in_buf, to = ((north_out, south_in, lat + 1), (south_out, north_in, lat - 1))[side]
        return pltpu.make_async_remote_copy(
            src_ref=out_buf.at[step],
            dst_ref=in_buf.at[step],
            send_sem=lat_send.at[side],
            recv_sem=lat_recv.at[step % 2, side],
            device_id=(lon, to),
            device_id_type=MESH,
        )

    MIDDLE = [(side_rows, middle)]
    ENDS = [(0, side_rows), (rows - side_rows, side_rows)]

    def spans_of(k):
        return ENDS if k == ends_chunk else [(side_rows + k * piece, piece)]

    def join(parts):
        return parts[0] if len(parts) == 1 else jnp.concatenate(parts, axis=0)

    def read(b, c, t, spans, shift=0):
        return join([field[b, c, t, PAD + at + shift : PAD + at + shift + n, :] for at, n in spans])

    def write(b, c, t, spans, value):
        done = 0
        for at, n in spans:
            field[b, c, t, PAD + at : PAD + at + n, :] = value[done : done + n]
            done += n

    def table(ref, i, spans):
        return join([ref[i, at : at + n, :] for at, n in spans])

    def rounded_at(c, k):
        return c * piece if k == ends_chunk else middle_at + c * middle + k * piece

    def mixed(lane_of, first, fifth, third):
        fifths = jnp.where(lane_of < cut_w + inside, turn(fifth, cut_w), turn(fifth, 64))
        return jnp.where(lane_of < cut_w, first, jnp.where(lane_of < cut_e, fifths, third))

    def pack_east(step, k, rest, zero, four):
        buffer = east_out.at[step, k]
        buffer[0:16, :] = zero
        buffer[16:32, :] = four
        low, high = rest[0:8], rest[8:16]
        buffer[32:40, :] = jnp.where(low_half, turn(low, late_w), turn(high, late_w + 64))
        buffer[40:41, :] = gather_rest(low, high, 64 + inside)

    def pack_west(step, k, one, two, three):
        buffer = west_out.at[step, k]
        buffer[0:16, :] = two
        buffer[16:32, :] = jnp.where(lane_piece < cut_e, three, one)
        low, high = one[0:8], one[8:16]
        buffer[32:40, :] = jnp.where(low_half, turn(low, -cut_w), turn(high, 64 - cut_w))
        buffer[40:41, :] = gather_rest(low, high, 64 + cut_w)

    def send_north(step):
        b = step % 2
        edge = slice(PAD + rows - 1, PAD + rows)
        for c in range(columns):
            for i in range(3):
                north_out[step, i, c : c + 1, :] = field[b, c, i, edge, :]

        @pl.when(has_north)
        def _():
            lat_copy(step, 0).start()

    def send_south(step):
        b = step % 2
        low = lane[0:1] < cut_y
        edge = slice(PAD, PAD + 1)
        for c in range(columns):
            south_out[step, 0, c : c + 1, :] = jnp.where(
                low, field[b, c, 5, edge, :], field[b, c, 2, edge, :]
            )
            for i in range(1, 3):
                south_out[step, i, c : c + 1, :] = field[b, c, i + 2, edge, :]

        @pl.when(has_south)
        def _():
            lat_copy(step, 1).start()

    def take_south(step):
        b = step % 2

        @pl.when(has_south)
        def _():
            lat_copy(step, 0).wait_recv()
            for c in range(columns):
                for i in range(3):
                    field[b, c, i, PAD - 1 : PAD, :] = south_in[step, i, c : c + 1, :]

    def take_north(step):
        b = step % 2
        edge = slice(PAD + rows, PAD + rows + 1)

        @pl.when(has_north)
        def _():
            lat_copy(step, 1).wait_recv()
            for c in range(columns):
                for i, t in ((0, 2), (1, 3), (2, 4), (0, 5)):
                    field[b, c, t, edge, :] = north_in[step, i, c : c + 1, :]

    def west_halo(step, k):
        buffer = west_in.at[step, k]
        main = buffer[32:40, :]
        rest = spread_rest(buffer[40:41, :], inside)
        shared = jnp.concatenate([turn(main, -late_w), turn(main, 64 - late_w)], axis=0)
        ends = [
            jnp.where(lane_eight < inside, turn(main, 64 * part + inside - 64), rest[part])
            for part in range(2)
        ]
        return {
            0: buffer[0:16, :],
            1: shared,
            3: shared,
            4: buffer[16:32, :],
            5: jnp.concatenate(ends, axis=0),
        }

    def east_halo(step, k):
        buffer = east_in.at[step, k]
        main, shared = buffer[32:40, :], buffer[16:32, :]
        rest = spread_rest(buffer[40:41, :], 64 + cut_w)
        moved = [
            jnp.where(lane_eight < 64 + cut_w, turn(main, cut_w - 64 * part), rest[part])
            for part in range(2)
        ]
        moved = jnp.concatenate(moved, axis=0)
        return {1: jnp.where(lane_piece < cut_e, moved, shared), 2: buffer[0:16, :], 3: shared}

    def advect(b, c, t, spans, from_west, from_east):
        lanes = lax.broadcasted_iota(jnp.int32, (sum(n for _, n in spans), LANES), 1)
        if t == 1:
            beside = jnp.where(lanes < cut_w, from_west(t), from_east(t))
        elif t == 2:
            beside = from_east(t)
        elif t == 3:
            beside = jnp.where(lanes < cut_e, from_east(t), from_west(t))
        else:
            beside = from_west(t)
        if t < 2:
            along = read(b, c, t, spans, -1)
        elif t == 2:
            along = jnp.where(lanes < cut_y, read(b, c, t, spans, -1), read(b, c, t, spans, 1))
        else:
            along = read(b, c, t, spans, 1)
        return (
            table(keep_x, t, spans) * read(b, c, t, spans)
            + table(push_x, t, spans) * beside
            + push_y[t, 0:1, :] * along
        )

    def advect_cell(step, c, spans, row, from_west, from_east):
        b = step % 2
        values, total = [], None
        n = sum(count for _, count in spans)
        for t in range(tiles):
            value = advect(b, c, t, spans, from_west, from_east)
            values.append(value)
            rounded[row : row + n, t * LANES : (t + 1) * LANES] = value.astype(jnp.bfloat16)
            total = value if total is None else total + value
        energy = jnp.sum(total, axis=1, keepdims=True) * mean_of
        growth = table(grow, c, spans) - (time_step * dissipation) * energy * table(scale, c, spans)
        return values, growth

    def advect_edge(step, side, k, row):
        b, spans = step % 2, spans_of(k)
        if side == 0:
            c, halo = 0, west_halo(step, k)
            return advect_cell(
                step, c, spans, row, lambda t: halo[t], lambda t: read(b, 1, t, spans)
            )
        c, halo = last, east_halo(step, k)
        return advect_cell(
            step, c, spans, row, lambda t: read(b, last - 1, t, spans), lambda t: halo[t]
        )

    def keep(c, spans, value):
        done = 0
        for at, n in spans:
            kept[c, at : at + n, :] = value[done : done + n]
            done += n

    def prepare(step, ends, group):
        b, spans = step % 2, ENDS if ends else MIDDLE
        deep = piece if ends else middle
        start = 0 if ends else middle_at
        for c in group:
            values, growth = advect_cell(
                step, c, spans, start + c * deep,
                lambda t, c=c: read(b, c - 1, t, spans), lambda t, c=c: read(b, c + 1, t, spans),
            )
            keep(c, spans, growth)
            for t in range(tiles):
                write(1 - b, c, t, spans, values[t])

    def edge(step, messages, filler=None):
        b = step % 2
        for side, k in messages:
            lon_copy(step, side, k).wait_recv()
        with jax.named_scope(f"edge#s={step}#k={messages[0][1]}#d={messages[0][0]}"):
            advected = []
            for side, k in messages:
                c, spans = 0 if side == 0 else last, spans_of(k)
                values, growth = advect_edge(step, side, k, rounded_at(c, k))
                keep(c, spans, growth)
                for t in range(tiles):
                    if t not in ((1, 2, 3), (0, 4))[side]:
                        write(1 - b, c, t, spans, values[t])
                if side == 1:
                    values[1] = mixed(lane_piece, values[1], values[5], values[3])
                advected.append((values, growth))
            products = []
            for side, k in messages:
                row = rounded_at(0 if side == 0 else last, k)
                part, at = (weights, LANES) if side == 0 else (east_weights, 0)
                products.append([
                    jnp.dot(
                        rounded[row : row + piece, :], part[:, at + i * LANES : at + (i + 1) * LANES],
                        preferred_element_type=jnp.float32,
                    )
                    for i in range(3)
                ])
            if filler is not None:
                filler()
            for (side, k), (values, growth), transfer in zip(messages, advected, products):
                c, spans = 0 if side == 0 else last, spans_of(k)
                sea_here = time_step * table(scale, c, spans)
                sent = ((1, 2, 3), (1, 0, 4))[side]
                new = [
                    growth * values[t] + sea_here * transfer[i]
                    for i, t in enumerate(sent)
                ]
                (pack_west, pack_east)[side](step + 1, k, *new)
                for t, value in list(zip(sent, new))[side:]:
                    write(1 - b, c, t, spans, value)
                lon_copy(step + 1, 1 - side, k).start()

    def block(step, ends):
        with jax.named_scope(f"block#s={step}#e={int(ends)}"):
            b, final = step % 2, step == STEPS - 1
            spans = ENDS if ends else MIDDLE
            deep = piece if ends else middle
            start = 0 if ends else middle_at
            first, count = (1, columns - 2) if final else (0, columns)
            transfer = jnp.dot(
                rounded[start + first * deep : start + (first + count) * deep, :], weights[...],
                preferred_element_type=jnp.float32,
            )
            for c in inner if final else range(columns):
                sea_here = time_step * table(scale, c, spans)
                growth = table(kept, c, spans)
                row = (c - first) * deep
                for t in (0, 4, 5) if c == 0 else (1, 2, 3, 5) if c == last else range(tiles):
                    moved = transfer[row : row + deep, t * LANES : (t + 1) * LANES]
                    value = growth * read(1 - b, c, t, spans) + sea_here * moved
                    if final:
                        emit(c, t, spans, value)
                    else:
                        write(1 - b, c, t, spans, value)

    def emit(c, t, spans, value):
        w, done = width(t), 0
        for at, n in spans:
            out_ref[c, at : at + n, t * LANES : t * LANES + w] = value[done : done + n, 0:w]
            done += n

    def finish(step, chunks):
        for side, k in chunks:
            lon_copy(step, side, k).wait_recv()
        with jax.named_scope(f"finish#n={len(chunks)}"):
            done = []
            for n, (side, k) in enumerate(chunks):
                done.append(advect_edge(step, side, k, n * piece))
            transfer = jnp.dot(
                rounded[0 : len(chunks) * piece, :], weights[...], preferred_element_type=jnp.float32
            )
            for n, (side, k) in enumerate(chunks):
                values, growth = done[n]
                c, spans = 0 if side == 0 else last, spans_of(k)
                sea_here = time_step * table(scale, c, spans)
                for t in range(tiles):
                    moved = transfer[n * piece : (n + 1) * piece, t * LANES : (t + 1) * LANES]
                    emit(c, t, spans, growth * values[t] + sea_here * moved)

    def by_side(step_of):
        @pl.when(odd)
        def _():
            step_of(1, 0)

        @pl.when(jnp.logical_not(odd))
        def _():
            step_of(0, 1)

    def take_column(c):
        for t in range(tiles):
            w = width(t)
            field[0, c, t, PAD : PAD + rows, 0:w] = (
                staged[c, :, t * LANES : t * LANES + w] * scale[c, :, 0:w]
            )

    for c in edges:
        field[0, c, tiles - 1, PAD : PAD + rows, :] = jnp.zeros((rows, LANES), jnp.float32)
    edge_loads.wait()
    for c in inner:
        loads[c].start()
    weight_load.start()
    for c in edges:
        take_column(c)
    for k in range(CHUNKS):
        spans = spans_of(k)
        pack_west(0, k, *(read(0, 0, t, spans) for t in (1, 2, 3)))
        mine = [read(0, last, t, spans) for t in range(tiles)]
        pack_east(0, k, mixed(lane_piece, mine[1], mine[5], mine[3]), mine[0], mine[4])

    with jax.named_scope("barrier"):
        heard = 2 + has_south.astype(jnp.int32) + has_north.astype(jnp.int32)
        pl.semaphore_wait(barrier, heard)

    def send_first(first, second):
        for k in range(CHUNKS):
            lon_copy(0, 1 - first, k).start()
        for k in [ends_chunk] + list(range(CHUNKS - 1)):
            lon_copy(0, 1 - second, k).start()

    by_side(send_first)

    for copy in small[1:]:
        copy.wait()
    forcing = wind_ref[...] * (1.0 - ice_ref[...].astype(jnp.float32))
    growth = jnp.transpose(sea * (1.0 + time_step * forcing))
    for c in range(columns):
        grow[c] = jnp.broadcast_to(growth[:, c : c + 1], (rows, LANES))
    row = lax.broadcasted_iota(jnp.int32, (rows, LANES), 0) + lat * rows
    latitude = (-60.0 + 120.0 * (row.astype(jnp.float32) + 0.5) / (rows * lats)) * (math.pi / 180.0)
    inverse = 1.0 / jnp.cos(latitude)
    for t in range(tiles):
        number = (lane + t * LANES).astype(jnp.float32)
        direction = jnp.floor((number + 0.5) * (1.0 / freqs))
        freq = number - direction * freqs
        speed = jnp.zeros((8, LANES), jnp.float32)
        for f in range(freqs):
            speed = jnp.where(freq == f, speed_ref[f], speed)
        real = (lane + t * LANES) < bins
        theta = (direction + 0.5) * (2.0 * math.pi / DIRS)
        along_y = jnp.where(real, jnp.abs(0.45 * jnp.sin(theta) * speed), 0.0)
        along_x = jnp.where(real, jnp.abs(0.225 * jnp.cos(theta) * speed), 0.0)
        push_y[t] = along_y
        along_x = along_x[0:1] * inverse
        push_x[t] = along_x
        keep_x[t] = 1.0 - along_x - along_y[0:1]

    zero_row = jnp.zeros((1, LANES), jnp.float32)
    for c in range(columns):
        for t in range(tiles):
            for b in range(2):
                field[b, c, t, PAD - 1 : PAD, :] = zero_row
                field[b, c, t, PAD + rows : PAD + rows + 1, :] = zero_row
        if c in inner:
            field[0, c, tiles - 1, PAD : PAD + rows, :] = jnp.zeros((rows, LANES), jnp.float32)

    inner_loads.wait()
    for c in inner:
        take_column(c)
    send_north(0)
    send_south(0)

    weight_load.wait()
    weights[...] = jnp.zeros_like(weights)
    weights[0:bins, 0:bins] = raw_weights[...]
    wide_lane = lax.broadcasted_iota(jnp.int32, (tiles * LANES, LANES), 1)
    east_weights[:, LANES : 2 * LANES] = weights[:, 0:LANES]
    east_weights[:, 2 * LANES : 3 * LANES] = weights[:, 4 * LANES : 5 * LANES]
    first, third, fifth = (
        weights[:, t * LANES : (t + 1) * LANES].astype(jnp.float32) for t in (1, 3, 5)
    )
    east_weights[:, 0:LANES] = mixed(wide_lane, first, fifth, third).astype(jnp.bfloat16)

    share = -(-len(inner) // (CHUNKS - 1))
    for step in range(STEPS):
        if step < STEPS - 1:

            def before(first, second):
                for k in range(CHUNKS - 1):
                    group = inner[k * share : (k + 1) * share]
                    edge(step, [(first, k)], lambda: prepare(step, False, group))
                take_south(step)
                take_north(step)
                edge(
                    step, [(first, ends_chunk), (second, ends_chunk)],
                    lambda: prepare(step, True, inner),
                )

            def after(first, second):
                for k in range(CHUNKS - 1):
                    edge(step, [(second, k)])

            by_side(before)
            block(step, True)
            send_south(step + 1)
            send_north(step + 1)

            @pl.when(lax.rem(lat, 2) == 1)
            def _():
                pl.delay(700)

            by_side(after)
            block(step, False)
        else:
            prepare(step, False, inner)
            block(step, False)
            take_south(step)
            take_north(step)
            prepare(step, True, inner)
            block(step, True)

            def close(first, second):
                finish(step, [(first, k) for k in range(CHUNKS - 1)])
                finish(step, [(first, ends_chunk)] + [(second, k) for k in range(CHUNKS)])

            by_side(close)
    for side, (out_buf, in_buf) in enumerate(((east_out, west_in), (west_out, east_in))):
        pltpu.make_async_remote_copy(
            src_ref=out_buf, dst_ref=in_buf, send_sem=lon_send.at[side],
            recv_sem=lon_recv.at[0, side, 0], device_id=(east, lat), device_id_type=MESH,
        ).wait_send()
    for side, (out_buf, in_buf, there) in enumerate(
        ((north_out, south_in, has_north), (south_out, north_in, has_south))
    ):

        @pl.when(there)
        def _():
            pltpu.make_async_remote_copy(
                src_ref=out_buf, dst_ref=in_buf, send_sem=lat_send.at[side],
                recv_sem=lat_recv.at[0, side], device_id=(east, lat), device_id_type=MESH,
            ).wait_send()


def on_device(spectrum, sea_mask, ice_flags, wind_forcing, group_speed, coupling):
    columns, rows, bins = spectrum.shape
    tiles = -(-bins // LANES)
    wide = tiles * LANES
    piece = rows // CHUNKS
    hbm = pl.BlockSpec(memory_space=pltpu.HBM)
    operands = (group_speed, sea_mask, ice_flags, wind_forcing, spectrum, coupling)
    f32 = jnp.float32
    lon_buffer = pltpu.VMEM((STEPS, CHUNKS, 41, LANES), f32)
    lat_buffer = pltpu.VMEM((STEPS, 3, columns, LANES), f32)
    return pl.pallas_call(
        functools.partial(kernel, group_speed.shape[0]),
        out_shape=jax.ShapeDtypeStruct(spectrum.shape, spectrum.dtype),
        in_specs=[hbm] * 6,
        out_specs=pl.BlockSpec(memory_space=pltpu.VMEM),
        scratch_shapes=[
            pltpu.SMEM(group_speed.shape, f32),
            pltpu.VMEM((columns, rows), jnp.int32),
            pltpu.VMEM((columns, rows), jnp.int32),
            pltpu.VMEM((columns, rows), f32),
            pltpu.VMEM((2, columns, tiles, rows + 2 * PAD, LANES), f32),
            pltpu.VMEM((columns, rows, bins), f32),
            pltpu.VMEM((wide, wide), jnp.bfloat16),
            pltpu.VMEM((wide, 3 * LANES), jnp.bfloat16),
            pltpu.VMEM((bins, bins), jnp.bfloat16),
            pltpu.VMEM((columns * rows, wide), jnp.bfloat16),
            pltpu.VMEM((columns, rows, LANES), f32),
            pltpu.VMEM((tiles, rows, LANES), f32),
            pltpu.VMEM((tiles, rows, LANES), f32),
            pltpu.VMEM((tiles, 8, LANES), f32),
            pltpu.VMEM((columns, rows, LANES), f32),
            pltpu.VMEM((columns, rows, LANES), f32),
            lon_buffer, lon_buffer, lon_buffer, lon_buffer,
            lat_buffer, lat_buffer, lat_buffer, lat_buffer,
            pltpu.SemaphoreType.DMA((2,)),
            pltpu.SemaphoreType.DMA((4,)),
            pltpu.SemaphoreType.DMA,
            pltpu.SemaphoreType.DMA((2,)),
            pltpu.SemaphoreType.DMA((2, 2, CHUNKS)),
            pltpu.SemaphoreType.DMA((2,)),
            pltpu.SemaphoreType.DMA((2, 2)),
        ],
        compiler_params=pltpu.CompilerParams(
            collective_id=0, has_side_effects=True, vmem_limit_bytes=32 * 1024 * 1024
        ),
    )(*(pltpu.with_memory_space_constraint(x, pltpu.HBM) for x in operands))


def solution(mesh):
    placed = (P("lon", "lat", None), P("lon", "lat"), P("lon", "lat"), P("lon", "lat"), P(), P())
    return jax.shard_map(
        on_device, mesh=mesh, in_specs=placed, out_specs=P("lon", "lat", None), check_vma=False
    )
```
